32 devices in a mesh: layer: 4 (over z), latent: 8 (over y, x, core).
Axes of the slice: x: 2, y: 2, z: 4, core: 2. Of those that a mesh axis runs over, the one named last changes fastest.
Arguments:
- activations: bfloat16 [4, 4096, 512], P('layer', 'latent'), may hold values from -6 to 6
- enc_weight: bfloat16 [4, 1024, 4096], P('layer', 'latent'), may hold values from -0.09375 to 0.09375
- enc_bias: float32 [4, 1024], P('layer', 'latent'), may hold values from -6 to 6
- dec_weight: bfloat16 [4, 1024, 4096], P('layer', 'latent'), may hold values from -0.25 to 0.25
- dec_bias: float32 [4, 4096], P('layer', 'latent'), may hold values from -3 to 3
- topk_index: int32 [4, 512, 8, 32], P('layer', None, 'latent'), may hold values from 0 to 127, all different within a row
Outputs:
- reconstruction: bfloat16 [4, 4096, 512], P('layer', 'latent')
- grad_enc: bfloat16 [4, 1024, 4096], P('layer', 'latent')
- grad_dec: bfloat16 [4, 1024, 4096], P('layer', 'latent')
The draws below stay inside these ranges and needn't reach their ends.
Inputs may be any that keep to these rules, and one draw needn't show every extreme that they name: `topk_index`: for each layer, token and latent shard the 32 entries are distinct.
All inputs are finite; a program needn't handle non-finite values.
Results may differ from the reference program's by a relative error of at most 0.018.
Values may be sent and summed in bfloat16 or wider, within the bound.
No kernel may reach another device: no remote copies, remote signals or barrier semaphores. Data moves between devices by JAX's collectives and lax.ppermute only.
A program may use at most 64 MiB of HBM per device.

```python
import jax
import jax.numpy as jnp
from jax import lax

D = 4096
LAT_DEV = 128
K_SHARD = 32
TOKENS = 512
LAYERS = 4
LAT_LAYER = 1024
N_LATENT = 8


def strengthened(values, key, source, target, blocks, factor):
    def block_of(dim):
        return (jnp.arange(values.shape[dim]) // (values.shape[dim] // blocks)).reshape((-1,) + (1,) * (values.ndim - 1 - dim))

    first = jax.random.permutation(key, blocks)[block_of(target)]
    other_side = (block_of(target) + blocks // 2) % blocks
    return jnp.where((block_of(source) == first) | (block_of(source) == other_side), factor * values, values)


def level_of(rng, shape, split, smallest, largest):
    level, own = 1.0, jax.random.fold_in(rng, 6)
    for axis_at, shards_of in split:
        steps = jnp.exp(jax.random.uniform(jax.random.fold_in(own, axis_at), (shards_of,), jnp.float32, smallest / len(split), largest / len(split)))
        level = level * jnp.repeat(steps, shape[axis_at] // shards_of).reshape([-1 if axis == axis_at else 1 for axis in range(len(shape))])
    return level


def different_ones(own_key, rows, number_of, top, lift):
    order = jax.random.permutation(jax.random.fold_in(own_key, 1), number_of)
    boost = order
    for power in range(3):
        boost = boost * boost // number_of
    boost = boost * lift // number_of
    chance = jax.random.randint(jax.random.fold_in(own_key, 2), (rows, number_of), 0, 4096) + boost
    fixed_rows = jax.random.permutation(jax.random.fold_in(own_key, 3), rows)[jnp.arange(number_of) % rows]
    chance = jnp.where(jnp.arange(rows)[:, None] == fixed_rows[None, :], 1 << 14, chance)
    score = chance * number_of + jnp.arange(number_of)
    return lax.top_k(score.astype(jnp.int32), top)[1].astype(jnp.int32)


def normal_values(own_key, extent, spread, limit, cuts=(), held_as=jnp.bfloat16):
    array = jax.random.normal(own_key, extent, jnp.float32) * spread
    if len(cuts) > 0:
        array = level_of(own_key, extent, cuts, -0.22, 0.18) * array
    return jnp.clip(array, min=-limit, max=limit).astype(held_as)


def noise_with(stream_key, dims, scale, most, split, heavy, kind=jnp.bfloat16):
    array = scale * jax.random.normal(stream_key, dims, jnp.float32)
    if split:
        array = array * level_of(stream_key, dims, split, -0.22, 0.18)
    return jnp.clip(strengthened(array, jax.random.fold_in(stream_key, 3), *heavy), -most, most).astype(kind)


def setup_inputs(seed: int = 0) -> dict:
    splits = jax.random.split(jax.random.key(seed), 7)
    return {
        "activations": normal_values(splits[0], (LAYERS, D, TOKENS), 1.0, 6.0, ((0, 4), (1, 8))),
        "enc_weight": normal_values(splits[1], (LAYERS, LAT_LAYER, D), D ** -0.5, 0.09375, ((0, 4), (1, 8))),
        "enc_bias": normal_values(splits[2], (LAYERS, LAT_LAYER), 1.0, 6.0, ((0, 4), (1, 8)), jnp.float32),
        "dec_weight": noise_with(splits[3], (LAYERS, LAT_LAYER, D), LAT_LAYER ** -0.5, 0.25, ((0, 4), (1, 8)), (1, 2, 8, 2.0)),
        "dec_bias": normal_values(splits[4], (LAYERS, D), 0.5, 3.0, ((0, 4), (1, 8)), jnp.float32),
        "topk_index": different_ones(splits[5], LAYERS * TOKENS * N_LATENT, LAT_DEV, K_SHARD, 0).reshape((LAYERS, TOKENS, N_LATENT, K_SHARD)),
    }


loss_scale = 0.0625


def layer_mask(index_layer):
    latent_ids = jnp.arange(LAT_DEV, dtype=jnp.int32)
    matched = jnp.any(index_layer[:, :, :, None] == latent_ids, axis=2)
    return matched.reshape(index_layer.shape[0], LAT_LAYER).T


def forward_layer(operands):
    acts_layer, enc_layer, bias_layer, dec_layer, index_layer = operands
    pre_act = jnp.dot(enc_layer, acts_layer, preferred_element_type=jnp.float32) + bias_layer[:, None]
    features = jnp.where(layer_mask(index_layer), pre_act, 0.0).astype(jnp.bfloat16)
    feat_blocks = features.reshape(N_LATENT, LAT_DEV, TOKENS)
    dec_blocks = dec_layer.reshape(N_LATENT, LAT_DEV, D)

    def add_block(running, blocks):
        partial_value = jnp.dot(blocks[1].T, blocks[0], preferred_element_type=jnp.float32)
        partial_value = lax.optimization_barrier(partial_value.astype(jnp.bfloat16)).astype(jnp.float32)
        return running + partial_value, None

    contrib, unused = lax.scan(add_block, jnp.zeros((D, TOKENS), jnp.float32), (feat_blocks, dec_blocks))
    return features, contrib


def backward_layer(operands):
    acts_layer, dec_layer, index_layer, feat_layer, grad_layer = operands
    grad_feat = jnp.dot(dec_layer, grad_layer, preferred_element_type=jnp.float32)
    grad_pre = jnp.where(layer_mask(index_layer), grad_feat, 0.0).astype(jnp.bfloat16)
    grad_dec = jnp.dot(feat_layer, grad_layer.T, preferred_element_type=jnp.float32).astype(jnp.bfloat16)
    grad_enc = jnp.dot(grad_pre, acts_layer.T, preferred_element_type=jnp.float32).astype(jnp.bfloat16)
    return grad_enc, grad_dec


def reference(activations, enc_weight, enc_bias, dec_weight, dec_bias, topk_index):
    features, contribs = lax.map(forward_layer, (activations, enc_weight, enc_bias, dec_weight, topk_index))
    rebuilt = dec_bias[:, :, None] + jnp.cumsum(contribs, axis=0)
    residue = (rebuilt - activations.astype(jnp.float32)) * loss_scale
    grad_contrib = jnp.cumsum(residue[::-1], axis=0)[::-1].astype(jnp.bfloat16)
    grad_enc, grad_dec = lax.map(backward_layer, (activations, dec_weight, topk_index, features, grad_contrib))
    return rebuilt.astype(jnp.bfloat16), grad_enc, grad_dec
```

```python
import functools

import jax
import jax.numpy as jnp
from jax import lax
from jax.experimental import pallas as pl
from jax.experimental.pallas import tpu as pltpu
from jax.sharding import PartitionSpec as P

loss_scale = 0.0625


VMEM = pl.BlockSpec(memory_space=pltpu.VMEM)


def call(body, outs, flops, nbytes, n_in):
    return pl.pallas_call(
        body,
        out_shape=outs,
        in_specs=[VMEM] * n_in,
        out_specs=jax.tree.map(lambda _: VMEM, outs),
        cost_estimate=pl.CostEstimate(flops=flops, bytes_accessed=nbytes, transcendentals=0),
    )


def shard_mask(index_rows, latent_count):
    latent_ids = jnp.arange(latent_count, dtype=jnp.int32)
    matched = index_rows.T[None, :, :] == latent_ids[:, None, None]
    return jnp.any(matched, axis=1)


def swap(value, axis, distance):
    size = lax.axis_size(axis)
    return lax.ppermute(value, axis, [(i, i ^ distance) for i in range(size)])


def arranged(weight, columns, width):
    rows = weight.shape[0]
    if width % 128:
        blocks = weight.reshape(rows, -1, width)
        return jnp.take(blocks, jnp.stack(columns), axis=1).reshape(rows, -1)

    def body(at_ref, in_ref, out_ref):
        for place in range(len(columns)):
            start = pl.multiple_of(at_ref[place] * width, width)
            out_ref[:, place * width : (place + 1) * width] = in_ref[:, pl.ds(start, width)]

    return pl.pallas_call(
        body,
        out_shape=jax.ShapeDtypeStruct((rows, len(columns) * width), weight.dtype),
        in_specs=[pl.BlockSpec(memory_space=pltpu.SMEM), VMEM],
        out_specs=VMEM,
        cost_estimate=pl.CostEstimate(flops=rows * 4096, bytes_accessed=rows * 16384, transcendentals=0),
    )(jnp.stack(columns).astype(jnp.int32), weight)


def placed(pieces, columns, width, total):
    rows = pieces[0].shape[0]
    if width % 128:
        blocks = jnp.concatenate(pieces, axis=1).reshape(rows, -1, width)
        order = jnp.zeros(len(columns), jnp.int32).at[jnp.stack(columns)].set(jnp.arange(len(columns)))
        return jnp.take(blocks, order, axis=1).reshape(rows, total)

    def body(at_ref, *refs):
        place = 0
        for piece in refs[:-1]:
            for block in range(piece.shape[1] // width):
                start = pl.multiple_of(at_ref[place] * width, width)
                refs[-1][:, pl.ds(start, width)] = piece[:, block * width : (block + 1) * width]
                place += 1

    return pl.pallas_call(
        body,
        out_shape=jax.ShapeDtypeStruct((rows, total), pieces[0].dtype),
        in_specs=[pl.BlockSpec(memory_space=pltpu.SMEM)] + [VMEM] * len(pieces),
        out_specs=VMEM,
        cost_estimate=pl.CostEstimate(flops=rows * 4096, bytes_accessed=rows * total * 4, transcendentals=0),
    )(jnp.stack(columns).astype(jnp.int32), *pieces)


def decode_chunk(dec_part, features, count):
    depth, wide = dec_part.shape
    tokens = features.shape[1]
    rows = wide // count

    def body(dec_ref, feat_ref, first_ref, *rest):
        for block in range(count):
            value = lax.dot_general(
                dec_ref[:, block * rows : (block + 1) * rows],
                feat_ref[...],
                (((0,), (0,)), ((), ())),
                preferred_element_type=jnp.float32,
            )
            if block == 0:
                first_ref[...] = value
            else:
                rest[block - 1][...] = value.astype(jnp.bfloat16)

    outs = [jax.ShapeDtypeStruct((rows, tokens), jnp.float32)]
    outs += [jax.ShapeDtypeStruct((rows, tokens), jnp.bfloat16)] * (count - 1)
    return call(body, outs, 2 * depth * wide * tokens, 2 * (depth * wide + depth * tokens + wide * tokens), 2)(
        dec_part, features
    )


def backward_chunk(dec_part, features, pieces, total):
    depth, wide = dec_part.shape
    tokens = features.shape[1]
    count = len(pieces)
    rows = wide // count
    own = depth // 2
    first = total is None

    def body(dec_ref, feat_ref, *refs):
        grads = refs[:count]
        total_ref, mine_ref, other_ref = refs[-3:]
        value = None if first else refs[count][...]
        for block in range(count):
            cut = slice(block * rows, (block + 1) * rows)
            grad = grads[block][...]
            part = jnp.dot(dec_ref[:, cut], grad, preferred_element_type=jnp.float32)
            value = part if value is None else value + part
            outer = lax.dot_general(
                feat_ref[...], grad, (((1,), (1,)), ((), ())), preferred_element_type=jnp.float32
            ).astype(jnp.bfloat16)
            mine_ref[:, cut] = outer[:own]
            other_ref[:, cut] = outer[own:]
        total_ref[...] = value

    outs = [
        jax.ShapeDtypeStruct((depth, tokens), jnp.float32),
        jax.ShapeDtypeStruct((own, wide), jnp.bfloat16),
        jax.ShapeDtypeStruct((own, wide), jnp.bfloat16),
    ]
    args = [dec_part, features, *pieces] + ([] if first else [total])
    return call(body, outs, 4 * depth * wide * tokens, 4 * (depth * wide + depth * tokens * 2), len(args))(*args)


def outer_blocks(grad_pre, pieces, columns):
    rows, tokens = grad_pre.shape
    wide = pieces[0].shape[0]

    def body(at_ref, grad_ref, *refs):
        for place in range(len(pieces)):
            start = pl.multiple_of(at_ref[place] * wide, wide)
            refs[-1][:, pl.ds(start, wide)] = lax.dot_general(
                grad_ref[...], refs[place][...], (((1,), (1,)), ((), ())), preferred_element_type=jnp.float32
            ).astype(jnp.bfloat16)

    count = len(pieces)
    return pl.pallas_call(
        body,
        out_shape=jax.ShapeDtypeStruct((rows, wide * count), jnp.bfloat16),
        in_specs=[pl.BlockSpec(memory_space=pltpu.SMEM)] + [VMEM] * (count + 1),
        out_specs=VMEM,
        cost_estimate=pl.CostEstimate(
            flops=2 * rows * wide * count * tokens, bytes_accessed=2 * count * wide * tokens, transcendentals=0
        ),
    )(jnp.stack(columns).astype(jnp.int32), grad_pre, *pieces)


def local(activations, enc_weight, enc_bias, dec_weight, dec_bias, topk_index):
    own_acts, encoder, decoder, bias = activations[0], enc_weight[0], dec_weight[0], dec_bias[0]
    latents, width = encoder.shape
    rows, tokens = own_acts.shape
    shards, layers = lax.axis_size("latent"), lax.axis_size("layer")
    here, layer = lax.axis_index("latent"), lax.axis_index("layer")
    chips, part = shards // 2, rows // layers
    chunks = min(layers, 4)
    per_chunk = layers // chunks

    same = [own_acts] + [swap(own_acts, "latent", 2 * k) for k in range(1, chips)]
    pieces = [None] * shards
    for k in range(chips):
        pieces[2 * k] = same[k]
        pieces[2 * k + 1] = swap(same[k], "latent", 1)

    def row_part(value, k):
        return lax.dynamic_slice_in_dim(value, (layer ^ k) * part, part, 0)

    acts_at = [row_part(own_acts, 0)] + [swap(row_part(own_acts, k), "layer", k) for k in range(1, layers)]
    bias_at = [row_part(bias, 0)] + [swap(row_part(bias, k), "layer", k) for k in range(1, layers)]

    def blocks_of(parity):
        return [
            ((here ^ (2 * k)) ^ parity) * layers + (layer ^ z) for z in range(layers) for k in range(chips)
        ]

    def by_chunk(value):
        if per_chunk == 1:
            return value
        value = value.reshape(latents, chunks, per_chunk, chips, part)
        return value.transpose(0, 1, 3, 2, 4).reshape(latents, -1)

    dec_own = by_chunk(arranged(decoder, blocks_of(0), part))
    dec_other = swap(by_chunk(arranged(decoder, blocks_of(1), part)), "latent", 1)
    dec_pair = jnp.concatenate([dec_own, dec_other], axis=0)
    chunk_wide = per_chunk * chips * part

    active = shard_mask(topk_index[0, :, 0, :], latents)
    pre_act = enc_bias[0][:, None]
    for k in range(shards):
        columns = lax.dynamic_slice_in_dim(encoder, (here ^ k) * rows, rows, 1)
        pre_act = pre_act + jnp.dot(columns, pieces[k], preferred_element_type=jnp.float32)
    features = jnp.where(active, pre_act, 0.0).astype(jnp.bfloat16)
    feat_pair = jnp.concatenate([features, swap(features, "latent", 1)], axis=0)

    contrib = [None] * layers
    for c in reversed(range(chunks)):
        blocks = decode_chunk(dec_pair[:, c * chunk_wide : (c + 1) * chunk_wide], feat_pair, chips)
        total = blocks[0]
        for k in range(1, chips):
            total = total + swap(blocks[k], "latent", 2 * k).astype(jnp.float32)
        for z in range(per_chunk):
            value = total[z * part : (z + 1) * part].astype(jnp.bfloat16)
            at = c * per_chunk + z
            contrib[at] = value if at == 0 else swap(value, "layer", at)

    contrib = [value.astype(jnp.float32) for value in contrib]
    offset = [b[:, None] - a.astype(jnp.float32) for a, b in zip(acts_at, bias_at)]
    rebuilt_parts, grad_parts = [], []
    for t in range(layers):
        target = layer ^ t
        rebuilt = bias_at[t][:, None]
        summed = jnp.zeros_like(contrib[0])
        for s in range(layers):
            source = layer ^ s
            rebuilt = rebuilt + jnp.where(source <= target, contrib[s], 0.0)
            times = (layers - jnp.maximum(source, target)).astype(jnp.float32)
            summed = summed + times * contrib[s] + jnp.where(source >= target, offset[s], 0.0)
        rebuilt_parts.append(rebuilt.astype(jnp.bfloat16))
        grad_parts.append((summed * loss_scale).astype(jnp.bfloat16))

    grads = [grad_parts[0]] + [swap(grad_parts[t], "layer", t) for t in range(1, layers)]
    rebuilts = [rebuilt_parts[0]] + [swap(rebuilt_parts[t], "layer", t) for t in range(1, layers)]

    total, mine, others = None, [], []
    for c in range(chunks):
        own = grads[c * per_chunk : (c + 1) * per_chunk]
        own = own[0] if per_chunk == 1 else jnp.concatenate(own, axis=0)
        gathered = [own] + [swap(own, "latent", 2 * k) for k in range(1, chips)]
        total, mine_part, other_part = backward_chunk(
            dec_pair[:, c * chunk_wide : (c + 1) * chunk_wide], feat_pair, gathered, total
        )
        mine.append(mine_part)
        others.append(swap(other_part, "latent", 1))
    grad_feat = total[:latents] + swap(total[latents:], "latent", 1)
    grad_pre = jnp.where(active, grad_feat, 0.0).astype(jnp.bfloat16)
    grad_enc = outer_blocks(grad_pre, pieces, [here ^ k for k in range(shards)])

    def order_of(parity):
        return [
            ((here ^ (2 * k)) ^ parity) * layers + (layer ^ (c * per_chunk + z))
            for c in range(chunks)
            for k in range(chips)
            for z in range(per_chunk)
        ]

    grad_dec = placed(mine + others, order_of(0) + order_of(1), part, width)

    reconstruction = jnp.zeros((rows, tokens), jnp.bfloat16)
    for t in range(layers):
        reconstruction = lax.dynamic_update_slice_in_dim(reconstruction, rebuilts[t], (layer ^ t) * part, 0)
    return reconstruction[None], grad_enc[None], grad_dec[None]


def solution(mesh):
    return jax.shard_map(
        local,
        mesh=mesh,
        in_specs=(
            P("layer", "latent", None),
            P("layer", "latent", None),
            P("layer", "latent"),
            P("layer", "latent", None),
            P("layer", "latent"),
            P("layer", None, "latent", None),
        ),
        out_specs=(
            P("layer", "latent", None),
            P("layer", "latent", None),
            P("layer", "latent", None),
        ),
        check_vma=False,
    )
```
